32 devices in a mesh: blk: 32 (over z, y, x, core).
Axes of the slice: x: 2, y: 2, z: 4, core: 2. Of those that a mesh axis runs over, the one named last changes fastest.
Arguments:
- panel_left: bfloat16 [64, 64, 2048], P('blk'), may hold values from -0.75 to 0.75
- panel_right: bfloat16 [64, 64, 2048], P('blk'), may hold values from -0.125 to 0.125
- ranks: int32 [64], P('blk'), may hold values from 1 to 64
- rhs: float32 [64, 64, 2048], P('blk'), may hold values from -6 to 6
- pivot_left: bfloat16 [2048, 64], P('blk'), may hold values from -0.75 to 0.75
- pivot_right: bfloat16 [2048, 64], P('blk'), may hold values from -6 to 6
- finished: float32 [2048, 64], P('blk'), may hold values from -6 to 6
- pivot_rhs: float32 [2048, 64], P('blk'), may hold values from -6 to 6
- diag_inverse: float32 [2048, 2048], P('blk'), as said below
Outputs:
- new_left: bfloat16 [64, 64, 2048], P('blk')
- new_rhs: float32 [64, 64, 2048], P('blk')
- next_solution: float32 [2048, 64], P('blk')
The draws below stay inside these ranges and needn't reach their ends.
Inputs may be any that keep to these rules, and one draw needn't show every extreme that they name: diag_inverse is lower triangular with diagonal entries between 1 and 2.
All inputs are finite; a program needn't handle non-finite values.
Results may differ from the reference program's by a relative error of at most 0.0049.
Values sent between devices are 32-bit elements; how exact they have to be, the bound alone decides.
A program may use at most 64 MiB of HBM per device.

```python
import jax
import jax.numpy as jnp
from jax import lax

NB = 2048
KMAX = 64
NRHS = 64
TILES = 64


def draw_diag_inverse(key, part):
    first = jax.random.fold_in(key, 11)
    second = jax.random.fold_in(key, 12)
    lower = jax.random.normal(first, (NB, NB), jnp.float32) * NB ** (-0.5)
    lower = jnp.tril(lower, -1)
    diag_vals = jax.random.uniform(second, (NB,), jnp.float32, 1.0, 2.0)
    return lower + jnp.diag(diag_vals)


def plant(values, rng, smallest, high):
    index_at = [jax.random.randint(jax.random.fold_in(rng, axis), (), 0, length) for axis, length in enumerate(values.shape)]
    widest = values.shape.index(max(values.shape))
    neighbour = index_at[:widest] + [(index_at[widest] + 1) % values.shape[widest]] + index_at[widest + 1:]
    return values.at[tuple(index_at)].set(smallest).at[tuple(neighbour)].set(high)


def block_scale(rng, dims, shards, smallest, high):
    level, own = 1.0, jax.random.fold_in(rng, 6)
    for position, parts in shards:
        steps = jnp.exp(jax.random.uniform(jax.random.fold_in(own, position), (parts,), jnp.float32, smallest / len(shards), high / len(shards)))
        level = level * jnp.repeat(steps, dims[position] // parts).reshape([-1 if axis == position else 1 for axis in range(len(dims))])
    return level


def noise(rng, extent, scale, limit, split=(), kind=jnp.bfloat16):
    level = block_scale(rng, extent, split, -0.22, 0.18) if split else 1.0
    drawn = jax.random.normal(rng, extent, jnp.float32) * scale * level
    return jnp.minimum(jnp.maximum(drawn, -limit), limit).astype(kind)


def setup_inputs(seed: int = 0) -> dict:
    seeds = jax.random.split(jax.random.key(seed), 10)
    return {
        "panel_left": noise(seeds[0], (TILES, KMAX, NB), KMAX ** -0.5, 0.75, ((0, 32),)),
        "panel_right": noise(seeds[1], (TILES, KMAX, NB), NB ** -0.5, 0.125, ((0, 32),)),
        "ranks": plant(jax.random.randint(seeds[2], (TILES,), 1, KMAX + 1), jax.random.fold_in(seeds[2], 1), 1, KMAX).astype(jnp.int32),
        "rhs": noise(seeds[3], (TILES, NRHS, NB), 1.0, 6.0, ((0, 32),), jnp.float32),
        "pivot_left": noise(seeds[4], (NB, KMAX), KMAX ** -0.5, 0.75, ((0, 32),)),
        "pivot_right": noise(seeds[5], (NB, KMAX), 1.0, 6.0, ((0, 32),)),
        "finished": noise(seeds[6], (NB, NRHS), 1.0, 6.0, ((0, 32),), jnp.float32),
        "pivot_rhs": noise(seeds[7], (NB, NRHS), 1.0, 6.0, ((0, 32),), jnp.float32),
        "diag_inverse": draw_diag_inverse(jax.random.fold_in(seeds[9], 71), 0),
    }


HIGH = lax.Precision.HIGHEST


def reference(panel_left, panel_right, ranks, rhs, pivot_left, pivot_right, finished, pivot_rhs, diag_inverse):
    columns = jnp.arange(KMAX, dtype=jnp.int32)
    pivot_wide = pivot_right.astype(jnp.float32)

    def one_tile(items):
        left, right, rank, right_side = items
        mask = (columns < rank).astype(jnp.bfloat16)
        left_m = (left * mask[:, None]).astype(jnp.float32)
        right_m = (right * mask[:, None]).astype(jnp.float32)
        gram = jnp.dot(right_m, pivot_wide, precision=HIGH).astype(jnp.bfloat16)
        proj = jnp.dot(right_m, finished, precision=HIGH)
        newl = jnp.dot(gram.astype(jnp.float32).T, left_m, precision=HIGH).astype(jnp.bfloat16)
        newr = right_side - jnp.dot(proj.T, left_m, precision=HIGH)
        return newl, newr

    new_left, new_rhs = lax.map(one_tile, (panel_left, panel_right, ranks, rhs))
    pivot_proj = jnp.dot(pivot_wide.T, finished, precision=HIGH)
    pivot_new = pivot_rhs - jnp.dot(pivot_left.astype(jnp.float32), pivot_proj, precision=HIGH)
    next_solution = jnp.dot(diag_inverse, pivot_new, precision=HIGH)
    return new_left, new_rhs, next_solution
```

```python
import functools

import jax
import jax.numpy as jnp
from jax import lax
from jax.experimental import pallas as pl
from jax.experimental.pallas import tpu as pltpu
from jax.sharding import PartitionSpec as P

MESH = pl.DeviceIdType.MESH
F32 = jnp.float32
BF16 = jnp.bfloat16


def factors(n):
    side = 1
    while (side * 2) ** 3 * 2 <= n and n % (2 * (side * 2) ** 2) == 0:
        side *= 2
    return n // (2 * side * side), side


def gather_kernel(
    n,
    right_any,
    diag_any,
    pr_ref,
    fin_ref,
    pl_ref,
    prhs_ref,
    prod_ref,
    next_ref,
    buf,
    right_v,
    diag_v,
    in_sem,
    send_sem,
    recv_sem,
):
    deep, side = factors(n)
    me = lax.axis_index("blk")
    core = me % 2
    dx = (me // 2) % side
    dy = (me // (2 * side)) % side
    z = me // (2 * side * side)
    s1 = 2 + core * (2 * side - 2)
    s2 = 2 * side - core * (2 * side - 2)
    f = dx + core * (dy - dx)
    g = dy + core * (dx - dy)

    def block(zz, ff, gg, cc=core):
        return zz * (2 * side * side) + ff * s1 + gg * s2 + cc

    load_right = pltpu.make_async_copy(right_any, right_v, in_sem.at[0])
    load_diag = pltpu.make_async_copy(diag_any, diag_v, in_sem.at[1])
    load_right.start()
    load_diag.start()
    half = pr_ref.shape[1]
    buf[0, me] = jnp.concatenate([pr_ref[...].astype(F32), fin_ref[...]], axis=1)
    buf[1, me] = jnp.concatenate([pl_ref[...].astype(F32), prhs_ref[...]], axis=1)

    def around(digit, size):
        order = sorted(range(1, size), key=lambda d: min(d, size - d))
        return [(digit + d) % size for d in order]

    zs, fs, gs = around(z, deep), around(f, side), around(g, side)
    partner = me + 1 - 2 * core
    z_to = [block(zz, f, g) for zz in zs]
    f_to = [block(z, ff, g) for ff in fs]
    g_to = [block(z, f, gg) for gg in gs]

    barrier = pltpu.get_barrier_semaphore()
    everyone = z_to + f_to + g_to + [partner]
    for peer in everyone:
        pl.semaphore_signal(barrier, inc=1, device_id=(peer,), device_id_type=MESH)
    pl.semaphore_wait(barrier, len(everyone))

    sent = []

    def copy(p, blk, to, slot):
        return pltpu.make_async_remote_copy(
            src_ref=buf.at[p, blk],
            dst_ref=buf.at[p, blk],
            send_sem=send_sem.at[p, slot],
            recv_sem=recv_sem.at[p, blk],
            device_id=(to,),
            device_id_type=MESH,
        )

    counts = [0, 0]

    def send(p, blk, to):
        c = copy(p, blk, to, counts[p])
        counts[p] += 1
        c.start()
        sent.append(c)

    def arrive(p, blk):
        copy(p, blk, partner, 0).wait_recv()

    def forward(p, blk, targets):
        for to in targets:
            send(p, blk, to)

    def own(p):
        forward(p, me, z_to + f_to + g_to + [partner])

    def stage_z(p):
        for zz in zs:
            blk = block(zz, f, g)
            arrive(p, blk)
            forward(p, blk, f_to + g_to + [partner])

    def stage_f(p):
        for zz in [z] + zs:
            for ff in fs:
                blk = block(zz, ff, g)
                arrive(p, blk)
                forward(p, blk, g_to + [partner])

    def stage_g(p):
        for ff in [f] + fs:
            for zz in [z] + zs:
                for gg in gs:
                    blk = block(zz, ff, gg)
                    arrive(p, blk)
                    forward(p, blk, [partner])

    def stage_core(p):
        for gg in [g] + gs:
            for ff in [f] + fs:
                for zz in [z] + zs:
                    blk = zz * (2 * side * side) + ff * s1 + gg * s2 + 1 - core
                    arrive(p, blk)

    own(0)
    own(1)
    stage_z(0)
    stage_f(0)
    stage_z(1)
    stage_g(0)
    stage_f(1)
    stage_core(0)

    rows = n * buf.shape[2]
    solved = buf[0].reshape(rows, 2 * half).astype(BF16)
    load_right.wait()
    tiles, kmax, width = right_v.shape
    prod_ref[...] = jnp.dot(right_v[...].reshape(tiles * kmax, width), solved, preferred_element_type=F32)
    cross = lax.dot_general(solved, solved, (((0,), (0,)), ((), ())), preferred_element_type=F32)
    at_row = lax.broadcasted_iota(jnp.int32, cross.shape, 0)
    at_lane = lax.broadcasted_iota(jnp.int32, cross.shape, 1)
    weight = jnp.where((at_row < half) & (at_lane >= half), cross, 0.0).astype(BF16)
    load_diag.wait()

    stage_g(1)
    stage_core(1)
    both = buf[1].reshape(rows, 2 * half)
    update = jnp.dot(both.astype(BF16), weight, preferred_element_type=F32)
    pivot_new = (both - update).astype(BF16)
    answer = jnp.dot(diag_v[...].astype(BF16), pivot_new, preferred_element_type=F32)
    next_ref[...] = answer[:, half:]
    for c in sent:
        c.wait_send()


def tile_kernel(ranks_ref, prod_ref, left_ref, rhs_ref, next_in, nl_ref, nr_ref, next_out):
    t = pl.program_id(0)
    kmax = left_ref.shape[1]
    half = nl_ref.shape[1]
    rank = ranks_ref[t]
    prod = prod_ref[...]
    prod = jnp.where(lax.broadcasted_iota(jnp.int32, prod.shape, 0) < rank, prod, 0.0)
    coef = prod.T.astype(BF16)
    left = left_ref[0]
    keep = lax.broadcasted_iota(jnp.int32, left.shape, 0) < rank
    left_m = jnp.where(keep, left, jnp.zeros_like(left))
    out = jnp.dot(coef, left_m, preferred_element_type=F32)
    nl_ref[0] = out[:half].astype(nl_ref.dtype)
    nr_ref[0] = rhs_ref[0] - out[half:]
    next_out[...] = next_in[...]


def solution(mesh):
    n = mesh.shape["blk"]

    def shards(panel_left, panel_right, ranks, rhs, pivot_left, pivot_right, finished, pivot_rhs, diag_inverse):
        tiles, kmax, width = panel_left.shape
        rows, half = finished.shape
        vmem = pl.BlockSpec(memory_space=pltpu.VMEM)
        hbm = pl.BlockSpec(memory_space=pl.ANY)
        deep, side = factors(n)
        steps = (deep - 1) + deep * (side - 1) + deep * side * (side - 1) + deep * side * side
        prod, nxt = pl.pallas_call(
            functools.partial(gather_kernel, n),
            out_shape=(
                jax.ShapeDtypeStruct((tiles * kmax, 2 * half), F32),
                jax.ShapeDtypeStruct((rows, half), F32),
            ),
            in_specs=[hbm, hbm, vmem, vmem, vmem, vmem],
            out_specs=(vmem, vmem),
            scratch_shapes=[
                pltpu.VMEM((2, n, rows, 2 * half), F32),
                pltpu.VMEM(panel_right.shape, BF16),
                pltpu.VMEM(diag_inverse.shape, F32),
                pltpu.SemaphoreType.DMA((2,)),
                pltpu.SemaphoreType.DMA((2, steps)),
                pltpu.SemaphoreType.DMA((2, n)),
            ],
            compiler_params=pltpu.CompilerParams(
                collective_id=0, has_side_effects=True, vmem_limit_bytes=32 * 1024 * 1024
            ),
        )(panel_right, diag_inverse, pivot_right, finished, pivot_left, pivot_rhs)

        cut = 2 if width % 256 == 0 else 1
        chunk = width // cut
        new_left, new_rhs, next_solution = pl.pallas_call(
            tile_kernel,
            grid=(tiles, cut),
            out_shape=(
                jax.ShapeDtypeStruct((tiles, half, width), BF16),
                jax.ShapeDtypeStruct((tiles, half, width), F32),
                jax.ShapeDtypeStruct((rows, half), F32),
            ),
            in_specs=[
                pl.BlockSpec(memory_space=pltpu.SMEM),
                pl.BlockSpec((kmax, 2 * half), lambda t, w: (t, 0)),
                pl.BlockSpec((1, kmax, chunk), lambda t, w: (t, 0, w)),
                pl.BlockSpec((1, half, chunk), lambda t, w: (t, 0, w)),
                pl.BlockSpec((rows, half), lambda t, w: (0, 0)),
            ],
            out_specs=(
                pl.BlockSpec((1, half, chunk), lambda t, w: (t, 0, w)),
                pl.BlockSpec((1, half, chunk), lambda t, w: (t, 0, w)),
                pl.BlockSpec((rows, half), lambda t, w: (0, 0)),
            ),
        )(ranks, prod, panel_left, rhs, nxt)
        return new_left, new_rhs, next_solution

    in_specs = (
        P("blk", None, None),
        P("blk", None, None),
        P("blk"),
        P("blk", None, None),
        P("blk", None),
        P("blk", None),
        P("blk", None),
        P("blk", None),
        P("blk", None),
    )
    out_specs = (P("blk", None, None), P("blk", None, None), P("blk", None))
    return jax.shard_map(shards, mesh=mesh, in_specs=in_specs, out_specs=out_specs, check_vma=False)
```

```python
import functools

import jax
import jax.numpy as jnp
from jax import lax
from jax.experimental import pallas as pl
from jax.experimental.pallas import tpu as pltpu
from jax.sharding import PartitionSpec as P

MESH = pl.DeviceIdType.MESH
F32 = jnp.float32
BF16 = jnp.bfloat16


def factors(n):
    side = 1
    while (side * 2) ** 3 * 2 <= n and n % (2 * (side * 2) ** 2) == 0:
        side *= 2
    return n // (2 * side * side), side


def gather_kernel(
    n,
    ranks_ref,
    left_hbm,
    right_hbm,
    rhs_hbm,
    pl_hbm,
    pr_hbm,
    fin_hbm,
    prhs_hbm,
    diag_hbm,
    nl_ref,
    nr_ref,
    next_ref,
    buf,
    left_v,
    right_v,
    diag_v,
    pl_v,
    pr_v,
    fin_v,
    prhs_v,
    in_sem,
    send_sem,
    recv_sem,
):
    deep, side = factors(n)
    me = lax.axis_index("blk")
    core = me % 2
    dx = (me // 2) % side
    dy = (me // (2 * side)) % side
    z = me // (2 * side * side)
    s1 = 2 + core * (2 * side - 2)
    s2 = 2 * side - core * (2 * side - 2)
    f = dx + core * (dy - dx)
    g = dy + core * (dx - dy)

    def block(zz, ff, gg, cc=core):
        return zz * (2 * side * side) + ff * s1 + gg * s2 + cc

    pairs = (
        (pr_hbm, pr_v),
        (fin_hbm, fin_v),
        (pl_hbm, pl_v),
        (prhs_hbm, prhs_v),
        (right_hbm, right_v),
        (left_hbm, left_v),
        (rhs_hbm, nr_ref),
        (diag_hbm, diag_v),
    )
    loads = [pltpu.make_async_copy(src, dst, in_sem.at[i]) for i, (src, dst) in enumerate(pairs)]
    for load in loads:
        load.start()
    half = pr_v.shape[1]

    def around(digit, size):
        order = sorted(range(1, size), key=lambda d: min(d, size - d))
        return [(digit + d) % size for d in order]

    zs, fs, gs = around(z, deep), around(f, side), around(g, side)
    partner = me + 1 - 2 * core
    z_to = [block(zz, f, g) for zz in zs]
    f_to = [block(z, ff, g) for ff in fs]
    g_to = [block(z, f, gg) for gg in gs]

    barrier = pltpu.get_barrier_semaphore()
    everyone = z_to + f_to + g_to + [partner]
    for peer in everyone:
        pl.semaphore_signal(barrier, inc=1, device_id=(peer,), device_id_type=MESH)
    for load in loads[:4]:
        load.wait()
    buf[0, me] = jnp.concatenate([pr_v[...].astype(F32), fin_v[...]], axis=1)
    buf[1, me] = jnp.concatenate([pl_v[...].astype(F32), prhs_v[...]], axis=1)
    pl.semaphore_wait(barrier, len(everyone))

    sent = []

    def copy(p, blk, to, slot):
        return pltpu.make_async_remote_copy(
            src_ref=buf.at[p, blk],
            dst_ref=buf.at[p, blk],
            send_sem=send_sem.at[p, slot],
            recv_sem=recv_sem.at[p, blk],
            device_id=(to,),
            device_id_type=MESH,
        )

    counts = [0, 0]

    def send(p, blk, to):
        c = copy(p, blk, to, counts[p])
        counts[p] += 1
        c.start()
        sent.append(c)

    def arrive(p, blk):
        copy(p, blk, partner, 0).wait_recv()

    def forward(p, blk, targets):
        for to in targets:
            send(p, blk, to)

    def own(p):
        forward(p, me, z_to + f_to + g_to + [partner])

    def stage_z(p):
        for zz in zs:
            blk = block(zz, f, g)
            arrive(p, blk)
            forward(p, blk, f_to + g_to + [partner])

    def stage_f(p):
        for zz in [z] + zs:
            for ff in fs:
                blk = block(zz, ff, g)
                arrive(p, blk)
                forward(p, blk, g_to + [partner])

    def stage_g(p):
        for ff in [f] + fs:
            for zz in [z] + zs:
                for gg in gs:
                    blk = block(zz, ff, gg)
                    arrive(p, blk)
                    forward(p, blk, [partner])

    def stage_core(p):
        for gg in [g] + gs:
            for ff in [f] + fs:
                for zz in [z] + zs:
                    blk = zz * (2 * side * side) + ff * s1 + gg * s2 + 1 - core
                    arrive(p, blk)

    own(0)
    own(1)
    stage_z(0)
    stage_f(0)
    stage_z(1)
    stage_g(0)
    stage_f(1)
    stage_core(0)

    rows = n * buf.shape[2]
    solved = buf[0].reshape(rows, 2 * half).astype(BF16)
    for load in loads[4:]:
        load.wait()
    tiles, kmax, width = right_v.shape
    prod = jnp.dot(right_v[...].reshape(tiles * kmax, width), solved, preferred_element_type=F32)
    cross = lax.dot_general(solved, solved, (((0,), (0,)), ((), ())), preferred_element_type=F32)
    at_row = lax.broadcasted_iota(jnp.int32, cross.shape, 0)
    at_lane = lax.broadcasted_iota(jnp.int32, cross.shape, 1)
    weight = jnp.where((at_row < half) & (at_lane >= half), cross, 0.0).astype(BF16)
    chunk = 512 if width % 512 == 0 else width
    for t in range(tiles):
        rank = ranks_ref[t]
        part = prod[t * kmax : (t + 1) * kmax]
        part = jnp.where(lax.broadcasted_iota(jnp.int32, part.shape, 0) < rank, part, 0.0)
        coef = part.T.astype(BF16)
        for w in range(0, width, chunk):
            left = left_v[t, :, w : w + chunk]
            keep = lax.broadcasted_iota(jnp.int32, left.shape, 0) < rank
            out = jnp.dot(coef, jnp.where(keep, left, jnp.zeros_like(left)), preferred_element_type=F32)
            nl_ref[t, :, w : w + chunk] = out[:half].astype(BF16)
            nr_ref[t, :, w : w + chunk] = nr_ref[t, :, w : w + chunk] - out[half:]

    stage_g(1)
    stage_core(1)
    both = buf[1].reshape(rows, 2 * half)
    update = jnp.dot(both.astype(BF16), weight, preferred_element_type=F32)
    pivot_new = (both - update).astype(BF16)
    answer = jnp.dot(diag_v[...].astype(BF16), pivot_new, preferred_element_type=F32)
    next_ref[...] = answer[:, half:]
    for c in sent:
        c.wait_send()


def solution(mesh):
    n = mesh.shape["blk"]

    def shards(panel_left, panel_right, ranks, rhs, pivot_left, pivot_right, finished, pivot_rhs, diag_inverse):
        tiles, kmax, width = panel_left.shape
        rows, half = finished.shape
        vmem = pl.BlockSpec(memory_space=pltpu.VMEM)
        hbm = pl.BlockSpec(memory_space=pltpu.HBM)
        deep, side = factors(n)
        steps = (deep - 1) + deep * (side - 1) + deep * side * (side - 1) + deep * side * side
        return pl.pallas_call(
            functools.partial(gather_kernel, n),
            out_shape=(
                jax.ShapeDtypeStruct((tiles, half, width), BF16),
                jax.ShapeDtypeStruct((tiles, half, width), F32),
                jax.ShapeDtypeStruct((rows, half), F32),
            ),
            in_specs=[pl.BlockSpec(memory_space=pltpu.SMEM)] + [hbm] * 8,
            out_specs=(vmem, vmem, vmem),
            scratch_shapes=[
                pltpu.VMEM((2, n, rows, 2 * half), F32),
                pltpu.VMEM(panel_left.shape, BF16),
                pltpu.VMEM(panel_right.shape, BF16),
                pltpu.VMEM(diag_inverse.shape, F32),
                pltpu.VMEM(pivot_left.shape, BF16),
                pltpu.VMEM(pivot_right.shape, BF16),
                pltpu.VMEM(finished.shape, F32),
                pltpu.VMEM(pivot_rhs.shape, F32),
                pltpu.SemaphoreType.DMA((8,)),
                pltpu.SemaphoreType.DMA((2, steps)),
                pltpu.SemaphoreType.DMA((2, n)),
            ],
            compiler_params=pltpu.CompilerParams(
                collective_id=0, has_side_effects=True, vmem_limit_bytes=67043328
            ),
        )(ranks, panel_left, panel_right, rhs, pivot_left, pivot_right, finished, pivot_rhs, diag_inverse)

    in_specs = (
        P("blk", None, None),
        P("blk", None, None),
        P("blk"),
        P("blk", None, None),
        P("blk", None),
        P("blk", None),
        P("blk", None),
        P("blk", None),
        P("blk", None),
    )
    out_specs = (P("blk", None, None), P("blk", None, None), P("blk", None))
    return jax.shard_map(shards, mesh=mesh, in_specs=in_specs, out_specs=out_specs, check_vma=False)
```

```python
import functools

import jax
import jax.numpy as jnp
from jax import lax
from jax.experimental import pallas as pl
from jax.experimental.pallas import tpu as pltpu
from jax.sharding import PartitionSpec as P

MESH = pl.DeviceIdType.MESH
F32 = jnp.float32
BF16 = jnp.bfloat16


def factors(n):
    side = 1
    while (side * 2) ** 3 * 2 <= n and n % (2 * (side * 2) ** 2) == 0:
        side *= 2
    return n // (2 * side * side), side


def gather_kernel(
    n,
    ranks_ref,
    left_hbm,
    right_hbm,
    rhs_hbm,
    pl_hbm,
    pr_hbm,
    fin_hbm,
    prhs_hbm,
    diag_hbm,
    nl_ref,
    nr_ref,
    next_ref,
    buf,
    left_v,
    right_v,
    diag_v,
    pl_v,
    pr_v,
    fin_v,
    prhs_v,
    in_sem,
    send_sem,
    recv_sem,
):
    deep, side = factors(n)
    me = lax.axis_index("blk")
    core = me % 2
    dx = (me // 2) % side
    dy = (me // (2 * side)) % side
    z = me // (2 * side * side)
    s1 = 2 + core * (2 * side - 2)
    s2 = 2 * side - core * (2 * side - 2)
    f = dx + core * (dy - dx)
    g = dy + core * (dx - dy)

    def block(zz, ff, gg, cc=core):
        return zz * (2 * side * side) + ff * s1 + gg * s2 + cc

    pairs = (
        (pr_hbm, pr_v),
        (fin_hbm, fin_v),
        (pl_hbm, pl_v),
        (prhs_hbm, prhs_v),
        (right_hbm, right_v),
        (left_hbm, left_v),
        (rhs_hbm, nr_ref),
        (diag_hbm, diag_v),
    )
    loads = [pltpu.make_async_copy(src, dst, in_sem.at[i]) for i, (src, dst) in enumerate(pairs)]
    for load in loads:
        load.start()
    half = pr_v.shape[1]

    def around(digit, size):
        order = sorted(range(1, size), key=lambda d: min(d, size - d))
        return [(digit + d) % size for d in order]

    zs, fs, gs = around(z, deep), around(f, side), around(g, side)
    partner = me + 1 - 2 * core
    z_to = [block(zz, f, g) for zz in zs]
    f_to = [block(z, ff, g) for ff in fs]
    g_to = [block(z, f, gg) for gg in gs]

    barrier = pltpu.get_barrier_semaphore()
    everyone = z_to + f_to + g_to + [partner]
    for peer in everyone:
        pl.semaphore_signal(barrier, inc=1, device_id=(peer,), device_id_type=MESH)
    for load in loads[:4]:
        load.wait()
    buf[0, me] = jnp.concatenate([pr_v[...].astype(F32), fin_v[...]], axis=1)
    buf[1, me] = jnp.concatenate([pl_v[...].astype(F32), prhs_v[...]], axis=1)
    pl.semaphore_wait(barrier, len(everyone))

    sent = []

    def copy(p, blk, to, slot):
        return pltpu.make_async_remote_copy(
            src_ref=buf.at[p, blk],
            dst_ref=buf.at[p, blk],
            send_sem=send_sem.at[p, slot],
            recv_sem=recv_sem.at[p, blk],
            device_id=(to,),
            device_id_type=MESH,
        )

    counts = [0, 0]

    def send(p, blk, to):
        c = copy(p, blk, to, counts[p])
        counts[p] += 1
        c.start()
        sent.append(c)

    def arrive(p, blk):
        copy(p, blk, partner, 0).wait_recv()

    def forward(p, blk, targets):
        for to in targets:
            send(p, blk, to)

    def own(p):
        forward(p, me, z_to + f_to + g_to + [partner])

    def stage_z(p):
        for zz in zs:
            blk = block(zz, f, g)
            arrive(p, blk)
            forward(p, blk, f_to + g_to + [partner])

    def stage_f(p):
        for zz in [z] + zs:
            for ff in fs:
                blk = block(zz, ff, g)
                arrive(p, blk)
                forward(p, blk, g_to + [partner])

    def stage_g(p):
        for ff in [f] + fs:
            for zz in [z] + zs:
                for gg in gs:
                    blk = block(zz, ff, gg)
                    arrive(p, blk)
                    forward(p, blk, [partner])

    def stage_core(p):
        for gg in [g] + gs:
            for ff in [f] + fs:
                for zz in [z] + zs:
                    blk = zz * (2 * side * side) + ff * s1 + gg * s2 + 1 - core
                    arrive(p, blk)

    own(0)
    own(1)
    stage_z(0)
    stage_f(0)
    stage_z(1)
    stage_g(0)
    stage_f(1)
    stage_core(0)

    rows = n * buf.shape[2]
    solved = buf[0].reshape(rows, 2 * half).astype(BF16)
    for load in loads[4:]:
        load.wait()
    tiles, kmax, width = right_v.shape
    prod = jnp.dot(right_v[...].reshape(tiles * kmax, width), solved, preferred_element_type=F32)
    cross = lax.dot_general(solved, solved, (((0,), (0,)), ((), ())), preferred_element_type=F32)
    at_row = lax.broadcasted_iota(jnp.int32, cross.shape, 0)
    at_lane = lax.broadcasted_iota(jnp.int32, cross.shape, 1)
    weight = jnp.where((at_row < half) & (at_lane >= half), cross, 0.0).astype(BF16)
    chunk = 512 if width % 512 == 0 else width
    for t in range(tiles):
        rank = ranks_ref[t]
        part = prod[t * kmax : (t + 1) * kmax]
        part = jnp.where(lax.broadcasted_iota(jnp.int32, part.shape, 0) < rank, part, 0.0)
        coef = part.T.astype(BF16)
        for w in range(0, width, chunk):
            left = left_v[t, :, w : w + chunk]
            keep = lax.broadcasted_iota(jnp.int32, left.shape, 0) < rank
            out = jnp.dot(coef, jnp.where(keep, left, jnp.zeros_like(left)), preferred_element_type=F32)
            nl_ref[t, :, w : w + chunk] = out[:half].astype(BF16)
            nr_ref[t, :, w : w + chunk] = nr_ref[t, :, w : w + chunk] - out[half:]

    stage_g(1)
    stage_core(1)
    both = buf[1].reshape(rows, 2 * half)
    update = jnp.dot(both.astype(BF16), weight, preferred_element_type=F32)
    pivot_new = (both - update).astype(BF16)
    answer = jnp.dot(diag_v[...].astype(BF16), pivot_new, preferred_element_type=F32)
    next_ref[...] = answer[:, half:]
    for c in sent:
        c.wait_send()


def write_kernel(nl_ref, nr_ref, next_ref, nl_out, nr_out, next_out, sem):
    pairs = ((nr_ref, nr_out), (nl_ref, nl_out), (next_ref, next_out))
    stores = [pltpu.make_async_copy(src, dst, sem.at[i]) for i, (src, dst) in enumerate(pairs)]
    for store in stores:
        store.start()
    for store in stores:
        store.wait()


def solution(mesh):
    n = mesh.shape["blk"]

    def shards(panel_left, panel_right, ranks, rhs, pivot_left, pivot_right, finished, pivot_rhs, diag_inverse):
        tiles, kmax, width = panel_left.shape
        rows, half = finished.shape
        vmem = pl.BlockSpec(memory_space=pltpu.VMEM)
        hbm = pl.BlockSpec(memory_space=pltpu.HBM)
        deep, side = factors(n)
        steps = (deep - 1) + deep * (side - 1) + deep * side * (side - 1) + deep * side * side
        arrays = (ranks, panel_left, panel_right, rhs, pivot_left, pivot_right, finished, pivot_rhs, diag_inverse)
        pinned = [pltpu.with_memory_space_constraint(a, pltpu.HBM) for a in arrays]
        results = pl.pallas_call(
            functools.partial(gather_kernel, n),
            out_shape=(
                jax.ShapeDtypeStruct((tiles, half, width), BF16),
                jax.ShapeDtypeStruct((tiles, half, width), F32),
                jax.ShapeDtypeStruct((rows, half), F32),
            ),
            in_specs=[pl.BlockSpec(memory_space=pltpu.SMEM)] + [hbm] * 8,
            out_specs=(vmem, vmem, vmem),
            scratch_shapes=[
                pltpu.VMEM((2, n, rows, 2 * half), F32),
                pltpu.VMEM(panel_left.shape, BF16),
                pltpu.VMEM(panel_right.shape, BF16),
                pltpu.VMEM(diag_inverse.shape, F32),
                pltpu.VMEM(pivot_left.shape, BF16),
                pltpu.VMEM(pivot_right.shape, BF16),
                pltpu.VMEM(finished.shape, F32),
                pltpu.VMEM(pivot_rhs.shape, F32),
                pltpu.SemaphoreType.DMA((8,)),
                pltpu.SemaphoreType.DMA((2, steps)),
                pltpu.SemaphoreType.DMA((2, n)),
            ],
            compiler_params=pltpu.CompilerParams(
                collective_id=0, has_side_effects=True, vmem_limit_bytes=40 * 1024 * 1024
            ),
        )(*pinned)
        return pl.pallas_call(
            write_kernel,
            out_shape=tuple(jax.ShapeDtypeStruct(r.shape, r.dtype) for r in results),
            in_specs=[vmem] * 3,
            out_specs=(hbm, hbm, hbm),
            scratch_shapes=[pltpu.SemaphoreType.DMA((3,))],
            compiler_params=pltpu.CompilerParams(vmem_limit_bytes=4 * 1024 * 1024),
        )(*results)

    in_specs = (
        P("blk", None, None),
        P("blk", None, None),
        P("blk"),
        P("blk", None, None),
        P("blk", None),
        P("blk", None),
        P("blk", None),
        P("blk", None),
        P("blk", None),
    )
    out_specs = (P("blk", None, None), P("blk", None, None), P("blk", None))
    return jax.shard_map(shards, mesh=mesh, in_specs=in_specs, out_specs=out_specs, check_vma=False)
```
